256 devices in a mesh: dp: 16 (over y_hi, x, core), seq: 16 (over y_lo, z).
Axes of the slice: x: 4, y: 4 (y_hi: 2, y_lo: 2; y = y_hi * 2 + y_lo), z: 8, core: 2. Of those that a mesh axis runs over, the one named last changes fastest.
Arguments:
- tokens: bfloat16 [16, 4096, 1280], P('dp', 'seq'), may hold values from -6 to 6
- tube_index: int32 [16, 4096], P('dp', 'seq'), may hold values from 0 to 16383
- counts: int32 [16, 16], P('dp', 'seq'), may hold values from 128 to 256
- qkv_weight: bfloat16 [1280, 3840], P('dp'), may hold values from -4 to 4
- proj_weight: bfloat16 [1280, 1280], P('dp'), may hold values from -0.15625 to 0.15625
- ctx_b: bfloat16 [16, 4096, 1280], P('dp', 'seq'), may hold values from -12 to 12
- cot_b: bfloat16 [16, 4096, 1280], P('dp', 'seq'), may hold values from -12 to 12
- b_counts: int32 [16, 16], P('dp', 'seq'), may hold values from 128 to 256
Outputs:
- out_a: bfloat16 [16, 4096, 1280], P('dp', 'seq')
- weight_grad: float32 [1280, 1280], P('dp')
The draws below stay inside these ranges and needn't reach their ends.
Inputs may be any that keep to these rules, and one draw needn't show every extreme that they name: `counts`: slots of a device's block past its count hold padding. `b_counts`: slots of a device's block past its count hold padding.
All inputs are finite; a program needn't handle non-finite values.
Results may differ from the reference program's by a relative error of at most 0.017.
Values may be sent and summed in bfloat16 or wider, within the bound.
No kernel may reach another device: no remote copies, remote signals or barrier semaphores. Data moves between devices by JAX's collectives and lax.ppermute only.
A program may use at most 128 MiB of HBM per device.

```python
import math
import jax
import jax.numpy as jnp
from jax import lax

D = 1280
HEADS = 16
CAP = 256
TUBES = 16384
CLIPS = 16
SLOTS = 4096
N_SEQ = 16


def draw_qkv_weight(key, part):
    base_key = jax.random.fold_in(jax.random.fold_in(key, 11), 0)
    weight = jax.random.normal(base_key, (D, 3 * D), jnp.float32) / jnp.sqrt(jnp.float32(D))
    return jnp.clip(weight, -4.0, 4.0).astype(jnp.bfloat16)


def draw_ctx_b(key, part):
    noise_key = jax.random.fold_in(jax.random.fold_in(key, 23), 0)
    values = jax.random.normal(noise_key, (CLIPS, SLOTS, D), jnp.float32)
    return jnp.clip(values, -12.0, 12.0).astype(jnp.bfloat16)


def draw_cot_b(key, part):
    noise_key = jax.random.fold_in(jax.random.fold_in(key, 37), 0)
    values = jax.random.normal(noise_key, (CLIPS, SLOTS, D), jnp.float32)
    return jnp.clip(values, -12.0, 12.0).astype(jnp.bfloat16)


def set_ends(drawn, key, smallest, top_value):
    longest = drawn.shape.index(max(drawn.shape))
    spots = []
    for shift in (0, 1):
        where = [jax.random.randint(jax.random.fold_in(key, axis), (), 0, length) for axis, length in enumerate(drawn.shape)]
        where[longest] = (where[longest] + shift) % drawn.shape[longest]
        spots.append(tuple(where))
    return drawn.at[spots[0]].set(smallest).at[spots[1]].set(top_value)


def steps_of(key, extent, shards, low, high):
    def one(dim, blocks):
        steps = jax.random.uniform(jax.random.fold_in(jax.random.fold_in(key, 6), dim), (blocks,), jnp.float32, low / len(shards), high / len(shards))
        return jnp.repeat(jnp.exp(steps), extent[dim] // blocks).reshape((-1,) + (1,) * (len(extent) - dim - 1))

    gain = one(*shards[0])
    for cut in shards[1:]:
        gain = gain * one(*cut)
    return gain


def normal_values(stream_key, dims, scale, limit, pieces=(), kind=jnp.bfloat16):
    entries = scale * jax.random.normal(stream_key, dims, jnp.float32)
    if pieces:
        entries = entries * steps_of(stream_key, dims, pieces, -0.22, 0.18)
    return jnp.clip(entries, -limit, limit).astype(kind)


def setup_inputs(seed: int = 0) -> dict:
    keys = jax.random.split(jax.random.key(seed), 9)
    tokens = normal_values(keys[0], (CLIPS, SLOTS, D), 1.0, 6.0, ((0, 16), (1, 16)))
    tube_index = set_ends(jax.random.randint(keys[1], (CLIPS, SLOTS), 0, TUBES), jax.random.fold_in(keys[1], 1), 0, TUBES - 1).astype(jnp.int32)
    counts = set_ends(jax.random.randint(keys[2], (CLIPS, N_SEQ), CAP // 2, CAP + 1), jax.random.fold_in(keys[2], 1), CAP // 2, CAP).astype(jnp.int32)
    qkv_weight = draw_qkv_weight(jax.random.fold_in(keys[8], 71), 0)
    proj_weight = normal_values(keys[4], (D, D), D ** -0.5, 0.15625, ((0, 16),))
    ctx_b = draw_ctx_b(jax.random.fold_in(keys[8], 71), 0)
    cot_b = draw_cot_b(jax.random.fold_in(keys[8], 71), 0)
    b_counts = set_ends(jax.random.randint(keys[7], (CLIPS, N_SEQ), CAP // 2, CAP + 1), jax.random.fold_in(keys[7], 1), CAP // 2, CAP).astype(jnp.int32)
    return dict(tokens=tokens, tube_index=tube_index, counts=counts, qkv_weight=qkv_weight, proj_weight=proj_weight, ctx_b=ctx_b, cot_b=cot_b, b_counts=b_counts)


def embed(tube_ids, model_width):
    half_width = model_width // 2
    positions = jnp.arange(half_width, dtype=jnp.float32)
    frequency = jnp.exp(positions * (-2.0 * math.log(10000.0) / model_width))
    angles = tube_ids.astype(jnp.float32)[:, None] * frequency[None, :]
    return jnp.concatenate([jnp.sin(angles), jnp.cos(angles)], axis=1)

def layer_norm(values):
    centered = values - lax.optimization_barrier(jnp.mean(values, axis=1, keepdims=True))
    spread = lax.optimization_barrier(jnp.mean(centered * centered, axis=1, keepdims=True))
    return centered * lax.rsqrt(spread + 1e-06)

def attend_head(head_in):
    query_rows, key_rows, value_rows, valid_keys = head_in
    seq_length = key_rows.shape[0]
    block_rows = math.gcd(seq_length, 512)
    head_width = query_rows.shape[1]
    score_scale = 1.0 / math.sqrt(head_width)
    blocked = query_rows.reshape(seq_length // block_rows, block_rows, head_width)

    def one_block(block_query):
        scores = jnp.dot(block_query, key_rows.T, preferred_element_type=jnp.float32) * score_scale
        scores = jnp.where(valid_keys[None, :], scores, -1e+30)
        top_score = lax.optimization_barrier(jnp.max(scores, axis=1, keepdims=True))
        exponent = jnp.exp(scores - top_score)
        weights = (exponent / lax.optimization_barrier(jnp.sum(exponent, axis=1, keepdims=True))).astype(jnp.bfloat16)
        return jnp.dot(weights, value_rows, preferred_element_type=jnp.float32).astype(jnp.bfloat16)
    return lax.map(one_block, blocked).reshape(seq_length, head_width)

def clip_layer(clip_in, qkv_weight, proj_weight):
    clip_tokens, clip_index, clip_counts = clip_in
    with_pos = clip_tokens.astype(jnp.float32) + embed(clip_index, D)
    normed = layer_norm(with_pos).astype(jnp.bfloat16)
    projected = jnp.dot(normed, qkv_weight, preferred_element_type=jnp.float32).astype(jnp.bfloat16)
    slot_ids = jnp.arange(CAP, dtype=jnp.int32)
    valid = (slot_ids[None, :] < clip_counts[:, None]).reshape(SLOTS)
    head_width = D // HEADS
    split_heads = projected.reshape(SLOTS, 3, HEADS, head_width).transpose(1, 2, 0, 3)
    valid_heads = jnp.broadcast_to(valid[None, :], (HEADS, SLOTS))
    context = lax.map(attend_head, (split_heads[0], split_heads[1], split_heads[2], valid_heads))
    context = context.transpose(1, 0, 2).reshape(SLOTS, D)
    output = with_pos + jnp.dot(context, proj_weight, preferred_element_type=jnp.float32)
    return output.astype(jnp.bfloat16)

def reference(tokens, tube_index, counts, qkv_weight, proj_weight, ctx_b, cot_b, b_counts):

    def per_clip(clip_in):
        return clip_layer(clip_in, qkv_weight, proj_weight)
    out_a = lax.map(per_clip, (tokens, tube_index, counts))
    slot_ids = jnp.arange(CAP, dtype=jnp.int32)
    b_valid = (slot_ids[None, None, :] < b_counts[:, :, None]).reshape(CLIPS * SLOTS, 1)
    masked_cot = jnp.where(b_valid, cot_b.reshape(CLIPS * SLOTS, D), jnp.zeros((), jnp.bfloat16))
    summed = lax.dot_general(ctx_b.reshape(CLIPS * SLOTS, D), masked_cot, (((0,), (0,)), ((), ())), preferred_element_type=jnp.float32)
    weight_grad = summed / math.sqrt(CLIPS * SLOTS)
    return (out_a, weight_grad)
```

```python
import functools
import math

import jax
import jax.numpy as jnp
from jax import lax
from jax.experimental import pallas as pl
from jax.experimental.pallas import tpu as pltpu
from jax.sharding import Mesh
from jax.sharding import PartitionSpec as P


HEADS = 16
YH, X, C, YL, Z = "dp_0", "dp_1", "dp_2", "seq_0", "seq_1"
DP = (YH, X, C)
SEQ = (YL, Z)
BF16 = jnp.bfloat16
F32 = jnp.float32


def shift(count, step):
    return [(i, (i + step) % count) for i in range(count)]


def swap_core(x):
    return lax.ppermute(x, C, [(0, 1), (1, 0)])


def swap_low(x):
    return lax.ppermute(x, YL, [(0, 1), (1, 0)])


def swap_cross(x):
    return lax.ppermute(x, (YH, YL), [(3, 0), (2, 1), (1, 2), (0, 3)])


def embed(tube_ids, model_width):
    half_width = model_width // 2
    positions = jnp.arange(half_width, dtype=F32)
    frequency = jnp.exp(positions * (-2.0 * math.log(10000.0) / model_width))
    angles = tube_ids.astype(F32)[:, None] * frequency[None, :]
    return jnp.concatenate([jnp.sin(angles), jnp.cos(angles)], axis=1)


def layer_norm(values):
    centered = values - jnp.mean(values, axis=1, keepdims=True)
    spread = jnp.mean(centered * centered, axis=1, keepdims=True)
    return centered * lax.rsqrt(spread + 1e-06)


def block_order(yh, x, c):
    ids = []
    for rc in range(2):
        for d in range(4):
            for ryh in range(2):
                ids.append((yh ^ ryh) * 8 + ((x - d) % 4) * 2 + (c ^ rc))
    return jnp.stack(ids).astype(jnp.int32)


def whole(*shape):
    return pl.BlockSpec(shape, lambda i, o: (0,) * len(shape))


def single(kernel, scalars, inputs, outputs, scratch):
    return pl.pallas_call(
        kernel,
        grid_spec=pltpu.PrefetchScalarGridSpec(
            num_scalar_prefetch=1,
            grid=(1,),
            in_specs=[whole(*x.shape) for x in inputs],
            out_specs=[whole(*o.shape) for o in outputs],
            scratch_shapes=scratch,
        ),
        out_shape=outputs,
    )(scalars, *inputs)


def turn_kernel(info, x_ref, o_ref, t_ref, p_ref):
    slots, width = x_ref.shape
    rows = width // HEADS
    t_ref[...] = x_ref[...].T
    for r in range(HEADS):
        start = pl.multiple_of(info[r] * rows, 16)
        p_ref[r * rows : (r + 1) * rows] = t_ref[pl.ds(start, rows), :]
    o_ref[:slots] = p_ref[...].T
    count = jnp.full((16, width), info[HEADS], jnp.int32)
    o_ref[slots:] = count.astype(F32).astype(BF16)


def turn_and_order(normed, order, count):
    slots, width = normed.shape
    out = jax.ShapeDtypeStruct((slots + 16, width), BF16)
    scratch = [pltpu.VMEM((width, slots), BF16), pltpu.VMEM((width, slots), BF16)]
    return single(turn_kernel, jnp.concatenate([order, count]), [normed], [out], scratch)[0]


def grad_kernel(order, factor, ab_ref, far_ref, own_ref, s1_ref, s2_ref, s3_ref, t_ref, m_ref):
    slots = ab_ref.shape[0] // 2
    rows = own_ref.shape[1]
    t_ref[:, :slots] = ab_ref[:slots, :].T
    t_ref[:, slots:] = far_ref[:slots, :].T
    m_ref[:slots, :] = ab_ref[slots:, :]
    m_ref[slots:, :] = far_ref[slots:, :]
    for r in range(8):
        start = pl.multiple_of(order[r] * rows, 16)
        part = jnp.dot(t_ref[pl.ds(start, rows), :], m_ref[...], preferred_element_type=F32) * factor
        if r < 2:
            own_ref[r] = part
        else:
            (s1_ref, s2_ref, s3_ref)[r // 2 - 1][r % 2] = part.astype(BF16)


def grad_pieces(order, factor, ab, far, rows):
    slots, width = ab.shape
    outs = [jax.ShapeDtypeStruct((2, rows, width), F32)] + [jax.ShapeDtypeStruct((2, rows, width), BF16)] * 3
    scratch = [pltpu.VMEM((width, slots), BF16), pltpu.VMEM((slots, width), BF16)]
    return single(lambda order, *refs: grad_kernel(order, factor, *refs), order, [ab, far], outs, scratch)


def project_kernel(_, ring_ref, far_ref, x_ref, y_ref, o_ref, *, kind, scale):
    half, outs = ring_ref.shape
    slots = x_ref.shape[0] - 16
    blocks = o_ref.shape[0]
    for k, v_ref in enumerate((x_ref, y_ref)):
        got = jnp.dot(v_ref[:slots, :half], ring_ref[...], preferred_element_type=F32)
        got = got + jnp.dot(v_ref[:slots, half:], far_ref[...], preferred_element_type=F32)
        if kind == "k":
            rows = outs // blocks
            lanes = slice(k * slots, (k + 1) * slots)
            o_ref[:, :rows, lanes] = got.astype(BF16).T.reshape(blocks, rows, slots)
            lane = lax.broadcasted_iota(jnp.int32, (16, slots), 1).astype(F32)
            row = lax.broadcasted_iota(jnp.int32, (16, slots), 0)
            bias = jnp.where((lane < v_ref[slots:, :slots].astype(F32)) | (row > 0), 0.0, -1e30).astype(BF16)
            o_ref[:, rows:, lanes] = jnp.broadcast_to(bias[None], (blocks, 16, slots))
        else:
            rows = outs // 2 // blocks
            lanes = slice(k * slots, (k + 1) * slots)
            o_ref[:, :rows, lanes] = got[:, : outs // 2].astype(BF16).T.reshape(blocks, rows, slots)
            query = (got[:, outs // 2 :] * scale).astype(BF16).T.reshape(blocks, rows, slots)
            part = slots // 2
            for h in range(2):
                at = (2 * h + k) * part
                o_ref[:, rows:, at : at + part] = query[:, :, h * part : (h + 1) * part]


def project(order, ring, far, near_x, far_x, z_count, kind, scale=None):
    pair = 2 * (near_x.shape[0] - 16)
    rows = ring.shape[1] // z_count + (16 if kind == "k" else 0)
    shapes = [jax.ShapeDtypeStruct((z_count, rows, pair), BF16)]
    kernel = functools.partial(project_kernel, kind=kind, scale=scale)
    return single(kernel, order, [ring, far, near_x, far_x], shapes, [])[0]


def attend_kernel(info, q_ref, k_ref, v_ref, *rest, key_block):
    blocks, tall, pair = k_ref.shape
    t_ref = rest[0] if len(rest) > 4 else None
    o_ref, kt_ref, ka_ref, va_ref = rest[-4:]
    group, head_width, part = q_ref.shape
    lanes = ka_ref.shape[1]
    extra = va_ref.shape[0] - head_width
    tile = group * part
    yl = info[0]

    @pl.when(pl.program_id(0) == 0)
    def _():
        kt_ref[...] = jnp.zeros_like(kt_ref)
        row = lax.broadcasted_iota(jnp.int32, (extra, pair), 0)
        for s in range(blocks):
            kt_ref[:tall, :] = k_ref[s]
            ka_ref[pl.ds(s * pair, pair), :] = kt_ref[...].T
            va_ref[:head_width, pl.ds(s * pair, pair)] = v_ref[s]
            va_ref[head_width:, pl.ds(s * pair, pair)] = jnp.where(row == 0, 1.0, 0.0).astype(BF16)

    ones = jnp.where(lax.broadcasted_iota(jnp.int32, (lanes - head_width, tile), 0) == 0, 1.0, 0.0)
    query = jnp.concatenate([q_ref[g] for g in range(group)], axis=1)
    query = jnp.concatenate([query, ones.astype(BF16)], axis=0)
    keys = ka_ref.shape[0]
    steps = keys // key_block

    def scores_of(j):
        return jnp.dot(ka_ref[pl.ds(j * key_block, key_block), :], query, preferred_element_type=F32)

    top = jnp.full((1, tile), -1e30, F32)
    total = jnp.zeros((head_width + extra, tile), F32)
    ahead = scores_of(0)
    for j in range(steps):
        scores = ahead
        if j + 1 < steps:
            ahead = scores_of(j + 1)
        new_top = jnp.maximum(top, jnp.max(scores, axis=0, keepdims=True))
        weights = jnp.exp2(scores - new_top).astype(BF16)
        got = jnp.dot(va_ref[:, pl.ds(j * key_block, key_block)], weights, preferred_element_type=F32)
        total = total * jnp.exp2(top - new_top) + got
        top = new_top
    context = (total[:head_width] / total[head_width : head_width + 1]).astype(BF16)
    half = part // 2
    for g in range(group):
        o_ref[yl, g, :head_width] = context[:, g * part : g * part + half]
        o_ref[1 - yl, g, :head_width] = context[:, g * part + half : (g + 1) * part]
    if t_ref is not None:
        o_ref[:, :, head_width:] = t_ref[...]


def attend(info, h, k, vq, tiles=None):
    blocks, _, pair = k.shape
    head_width = vq.shape[1] // 2
    part = pair // 2
    group = 4
    keys = blocks * pair
    in_specs = [
        pl.BlockSpec((group, head_width, part), lambda i, o: (i, 1, h)),
        whole(*k.shape),
        pl.BlockSpec((blocks, head_width, pair), lambda i, o: (0, 0, 0)),
    ]
    args = [vq, k, vq]
    rows = head_width
    if tiles is not None:
        extra = tiles.shape[2]
        in_specs.append(pl.BlockSpec((2, group, extra, 128), lambda i, o: (0, i, 0, 0)))
        args.append(tiles)
        rows += extra
    return pl.pallas_call(
        functools.partial(attend_kernel, key_block=512),
        grid_spec=pltpu.PrefetchScalarGridSpec(
            num_scalar_prefetch=1,
            grid=(blocks // group,),
            in_specs=in_specs,
            out_specs=pl.BlockSpec((2, group, rows, part // 2), lambda i, o: (0, i, 0, 0)),
            scratch_shapes=[
                pltpu.VMEM((128, pair), BF16),
                pltpu.VMEM((keys, 128), BF16),
                pltpu.VMEM((head_width + 16, keys), BF16),
            ],
        ),
        out_shape=jax.ShapeDtypeStruct((2, blocks, rows, part // 2), BF16),
        compiler_params=pltpu.CompilerParams(dimension_semantics=("arbitrary",)),
        name="attend",
    )(info, *args)


def tile_kernel(_, own_ref, got_ref, o_ref):
    rows, width = own_ref.shape
    total = (own_ref[...] + got_ref[...].astype(F32)).astype(BF16)
    across = width // 128
    per = o_ref.shape[2] // 16
    count = (rows // 16) * across
    for t in range(2 * o_ref.shape[1] * per):
        group, at = divmod(t, per)
        if t < count:
            r, l = divmod(t, across)
            piece = total[16 * r : 16 * r + 16, 128 * l : 128 * l + 128]
        else:
            piece = jnp.zeros((16, 128), BF16)
        o_ref[group // o_ref.shape[1], group % o_ref.shape[1], 16 * at : 16 * at + 16] = piece


def finish_kernel(order, c_ref, ring_ref, far_ref, w_ref, *refs):
    o_ref = refs[0]
    t_ref = refs[-1]
    half = ring_ref.shape[0]
    rows = half // 8
    for r in range(HEADS):
        t_ref[r * rows : (r + 1) * rows] = c_ref[order[r], :rows]
    context = t_ref[...].T
    mixed = jnp.dot(context[:, :half], ring_ref[...], preferred_element_type=F32)
    mixed = mixed + jnp.dot(context[:, half:], far_ref[...], preferred_element_type=F32)
    o_ref[...] = (w_ref[...] + mixed).astype(BF16)
    if len(refs) == 3:
        g_ref = refs[1]
        across = g_ref.shape[1] // 128
        per = (c_ref.shape[1] - rows) // 16
        for t in range((g_ref.shape[0] // 16) * across):
            group, at = divmod(t, per)
            r, l = divmod(t, across)
            piece = c_ref[group, rows + 16 * at : rows + 16 * at + 16]
            g_ref[16 * r : 16 * r + 16, 128 * l : 128 * l + 128] = piece.astype(F32)


def after(value, *others):
    return lax.optimization_barrier((value, *others))[0]


def x_ring(pieces):
    return [lax.ppermute(p, X, shift(4, d)) for d, p in zip((1, 2, 3), pieces)]


def on_device(tokens, tube_index, counts, qkv_weight, proj_weight, ctx_b, cot_b, b_counts):
    slots = tokens.shape[1]
    width = tokens.shape[2]
    z_count = lax.axis_size(Z)
    rows = qkv_weight.shape[0]
    head_width = width // HEADS
    half_width = width // 2
    yh, x, c, yl = (lax.axis_index(a) for a in (YH, X, C, YL))
    order = block_order(yh, x, c)

    def columns(part, side):
        return lax.dynamic_slice(qkv_weight, (0, part * width + side * half_width), (rows, half_width))

    near_k = columns(1, yl)
    cross_k = swap_cross(columns(1, 1 - yl))

    with_pos = tokens[0].astype(F32) + embed(tube_index[0], width)
    normed = layer_norm(with_pos).astype(BF16)
    turned = turn_and_order(normed, order, counts[0])
    other = swap_low(turned)

    def ring_of(pair, got):
        return jnp.stack([pair] + got).reshape(-1, pair.shape[2])

    pair_k = jnp.stack([near_k, cross_k])
    got_k = x_ring([pair_k] * 3)
    ring_k = ring_of(pair_k, got_k)
    far_k = swap_core(ring_k)

    rest = jnp.concatenate([columns(2, 1 - yl), columns(0, 1 - yl), proj_weight], axis=1)
    cross_rest = swap_cross(after(rest, pair_k))

    row_ids = lax.broadcasted_iota(jnp.int32, (slots, 1), 0)
    local_cot = after(cot_b[0], turned)
    masked_cot = jnp.where(row_ids < b_counts[0, 0], local_cot, jnp.zeros((), BF16))
    both_b = jnp.concatenate([ctx_b[0], masked_cot])
    far_b = swap_core(both_b)

    made_k = project(order, ring_k, far_k, turned, other, z_count, "k")
    keys = lax.all_to_all(made_k, Z, 0, 0, tiled=True)

    near_vq = jnp.concatenate([columns(2, yl), columns(0, yl)], axis=1)
    pair_vq = after(jnp.stack([near_vq, cross_rest[:, :width]]), *got_k)
    got_vq = x_ring([pair_vq] * 3)
    got_vq = list(lax.optimization_barrier((*got_vq, made_k))[:3])
    ring_vq = ring_of(pair_vq, got_vq)
    far_vq = swap_core(ring_vq)

    factor = 1.0 / math.sqrt(lax.axis_size(DP) * lax.axis_size(SEQ) * slots)
    targets = []
    for d in range(4):
        for ryh in range(2):
            targets.append((yh ^ ryh) * 8 + ((x + d) % 4) * 2 + c)
    own, *sends = grad_pieces(jnp.stack(targets).astype(jnp.int32), factor, both_b, after(far_b, made_k), rows)

    q_scale = math.log2(math.e) / math.sqrt(head_width)
    made_vq = project(order, ring_vq, after(far_vq, own), turned, other, z_count, "vq", q_scale)
    values = lax.all_to_all(made_vq, Z, 0, 0, tiled=True)

    got_g = x_ring(lax.optimization_barrier((*sends, *got_vq))[:3])
    for g in got_g:
        own = own + g.astype(F32)
    pair_p = after(jnp.stack([proj_weight, cross_rest[:, width:]]), *got_g)
    got_p = x_ring([pair_p] * 3)
    tiles = single(
        tile_kernel,
        order,
        [own[0], after(swap_cross(own[1]), pair_p)],
        [jax.ShapeDtypeStruct((2, z_count, 64, 128), BF16)],
        [],
    )[0]
    ring_p = ring_of(pair_p, got_p)
    far_p = swap_core(ring_p)

    half = slots // 2

    def finish(context, h, done=None):
        kernel = finish_kernel
        args = [context, ring_p, far_p, with_pos]
        specs = [
            whole(*context.shape),
            whole(*ring_p.shape),
            whole(*far_p.shape),
            pl.BlockSpec((half, width), lambda i, o: (h, 0)),
        ]
        outs = [jax.ShapeDtypeStruct((slots, width), BF16)]
        out_specs = [pl.BlockSpec((half, width), lambda i, o: (h, 0))]
        aliases = {}
        if done is not None:
            kernel = lambda order, c, r, f, w, d, *refs: finish_kernel(order, c, r, f, w, *refs)
            args.append(done)
            specs.append(pl.BlockSpec(memory_space=pl.ANY))
            outs.append(jax.ShapeDtypeStruct((rows, width), F32))
            out_specs.append(whole(rows, width))
            aliases = {5: 0}
        return pl.pallas_call(
            kernel,
            grid_spec=pltpu.PrefetchScalarGridSpec(
                num_scalar_prefetch=1,
                grid=(1,),
                in_specs=specs,
                out_specs=out_specs,
                scratch_shapes=[pltpu.VMEM((width, half), BF16)],
            ),
            out_shape=outs,
            input_output_aliases=aliases,
            name="finish",
        )(order, *args)

    info = yl.reshape(1).astype(jnp.int32)
    first = attend(info, 0, keys, values, tiles).reshape(HEADS, -1, half)
    first = lax.all_to_all(first, SEQ, 0, 0, tiled=True)
    second = attend(info, 1, keys, values).reshape(HEADS, -1, half)
    summed = first[:, head_width:].astype(F32).sum(0).astype(BF16)
    second = jnp.concatenate([second, jnp.broadcast_to(summed[None], (HEADS, 64, 128))], axis=1)
    second = lax.all_to_all(second, SEQ, 0, 0, tiled=True)
    out_first = finish(first, 0)[0]
    out_a, weight_grad = finish(second, 1, out_first)
    return (out_a[None], weight_grad)


def solution(mesh):
    split = Mesh(mesh.devices.reshape(2, 4, 2, 2, 8), ("dp_0", "dp_1", "dp_2", "seq_0", "seq_1"))
    return jax.shard_map(
        on_device,
        mesh=split,
        in_specs=(
            P(DP, SEQ, None),
            P(DP, SEQ),
            P(DP, SEQ),
            P(DP, None),
            P(DP, None),
            P(DP, SEQ, None),
            P(DP, SEQ, None),
            P(DP, SEQ),
        ),
        out_specs=(P(DP, SEQ, None), P(DP, None)),
        check_vma=False,
    )
```
